32 devices in a mesh: dp: 8 (over z, x), expert: 4 (over y, core).
Axes of the slice: x: 2, y: 2, z: 4, core: 2. Of those that a mesh axis runs over, the one named last changes fastest.
Arguments:
- local_grads: bfloat16 [8, 4, 4, 524288], P('dp', 'expert')
- master_weights: float32 [4, 4, 524288], P('expert', None, 'dp'), may hold values from -6 to 6
- first_moment: float32 [4, 4, 524288], P('expert', None, 'dp')
- second_moment: float32 [4, 4, 524288], P('expert', None, 'dp')
Outputs:
- new_params: bfloat16 [4, 4, 524288], P('expert')
- new_master: float32 [4, 4, 524288], P('expert', None, 'dp')
- new_first: float32 [4, 4, 524288], P('expert', None, 'dp')
- new_second: float32 [4, 4, 524288], P('expert', None, 'dp')
The draws below stay inside these ranges and needn't reach their ends.
All inputs are finite; a program needn't handle non-finite values.
Results may differ from the reference program's by a relative error of at most 0.0013.
Values may be sent and summed in bfloat16 or wider, within the bound.
A program may use at most 128 MiB of HBM per device.

```python
import jax
import jax.numpy as jnp
from jax import lax

LAYERS = 4
SHARD = 65536
EXPERTS = 4
FLAT = 524288
N_DP = 8


def unit_scale():
    return (EXPERTS * LAYERS * FLAT) ** (-0.5)


def profile_gains(key, block_top, jitter):
    replicas = FLAT // SHARD
    block_count = replicas * 4
    expert_rise = 1.0 + 2.0 * jnp.arange(EXPERTS, dtype=jnp.float32) / max(EXPERTS - 1, 1)
    expert_jitter = jnp.exp(jax.random.uniform(jax.random.fold_in(key, 11), (EXPERTS,), jnp.float32, -jitter, jitter))
    block_rise = 1.0 + block_top * jnp.arange(block_count, dtype=jnp.float32) / max(block_count - 1, 1)
    block_jitter = jnp.exp(jax.random.uniform(jax.random.fold_in(key, 12), (EXPERTS, LAYERS, block_count), jnp.float32, -jitter, jitter))
    blocks = (expert_rise * expert_jitter).reshape(EXPERTS, 1, 1) * block_rise.reshape(1, 1, block_count) * block_jitter
    return jnp.repeat(blocks, SHARD // 4, axis=2)


def draw_local_grads(key, part):
    replicas = FLAT // SHARD
    shape = (replicas, EXPERTS, LAYERS, FLAT)
    rough = jax.random.uniform(jax.random.fold_in(key, 7), (EXPERTS, LAYERS, FLAT), jnp.float32, 0.5, 1.5)
    gains = profile_gains(key, 2.0, 0.7)
    common = jax.random.normal(jax.random.fold_in(key, 3), (EXPERTS, LAYERS, FLAT), jnp.float32)
    single = jax.random.normal(jax.random.fold_in(key, 4), shape, jnp.float32)
    spread = 60.0
    centered = single - jnp.mean(single, axis=0, keepdims=True)
    values = (common[None] + spread * centered) * (gains * rough * unit_scale())[None]
    return values.astype(jnp.bfloat16)


def draw_first_moment(key, part):
    shape = (EXPERTS, LAYERS, FLAT)
    values = 0.3 * jax.random.normal(key, shape, jnp.float32)
    return values * unit_scale()


def draw_second_moment(key, part):
    shape = (EXPERTS, LAYERS, FLAT)
    low = 0.1
    logs = jax.random.uniform(key, shape, jnp.float32, jnp.log(low), 0.0)
    return jnp.exp(logs) * unit_scale() ** 2


def levels(own_key, extent, split, low, high):
    factor_of, own = 1.0, jax.random.fold_in(own_key, 6)
    for axis_at, shards_of in split:
        steps = jnp.exp(jax.random.uniform(jax.random.fold_in(own, axis_at), (shards_of,), jnp.float32, low / len(split), high / len(split)))
        factor_of = factor_of * jnp.repeat(steps, extent[axis_at] // shards_of).reshape([-1 if axis == axis_at else 1 for axis in range(len(extent))])
    return factor_of


def gaussian(own_key, shape, scale, bound, pieces=(), kind=jnp.bfloat16):
    gain = levels(own_key, shape, pieces, -0.22, 0.18) if pieces else 1.0
    result = jax.random.normal(own_key, shape, jnp.float32) * scale * gain
    return jnp.minimum(jnp.maximum(result, -bound), bound).astype(kind)


def setup_inputs(seed: int = 0) -> dict:
    key_of = jax.random.split(jax.random.key(seed), 5)
    local_grads = draw_local_grads(jax.random.fold_in(key_of[4], 71), 0)
    master_weights = gaussian(key_of[1], (EXPERTS, LAYERS, FLAT), 1.0, 6.0, ((0, 4), (2, 8)), jnp.float32)
    first_moment = draw_first_moment(jax.random.fold_in(key_of[4], 71), 0)
    second_moment = draw_second_moment(jax.random.fold_in(key_of[4], 71), 0)
    return dict(local_grads=local_grads, master_weights=master_weights, first_moment=first_moment, second_moment=second_moment)


beta_first = 0.9
beta_second = 0.95
correct_first = 1.0 - 0.9 ** 10
correct_second = 1.0 - 0.95 ** 10
learn_rate = 0.05
decay_rate = 0.1
clip_limit = 1.0
tiny_eps = 1e-08
norm_eps = 1e-06

def adam_update(gradient, master, first, second, clip_factor):
    scaled = clip_factor * gradient
    new_first = beta_first * first + (1.0 - beta_first) * scaled
    new_second = beta_second * second + (1.0 - beta_second) * scaled * scaled
    direction = new_first / correct_first / (jnp.sqrt(new_second / correct_second) + tiny_eps)
    new_master = master - learn_rate * (decay_rate * master + direction)
    return (new_master, new_first, new_second)

def reference(local_grads, master_weights, first_moment, second_moment):
    mean_grad = lax.optimization_barrier(jnp.sum(local_grads.astype(jnp.float32), axis=0)) / N_DP
    grad_norm = jnp.sqrt(jnp.sum(mean_grad * mean_grad))
    clip_factor = jnp.minimum(1.0, clip_limit / (grad_norm + norm_eps))
    new_master, new_first, new_second = adam_update(mean_grad, master_weights, first_moment, second_moment, clip_factor)
    return (new_master.astype(jnp.bfloat16), new_master, new_first, new_second)
```

```python
import functools

import jax
import jax.numpy as jnp
from jax import lax
from jax.experimental import pallas as pl
from jax.experimental.pallas import tpu as pltpu
from jax.sharding import PartitionSpec as P

beta_first = 0.9
beta_second = 0.95
correct_first = 1.0 - 0.9**10
correct_second = 1.0 - 0.95**10
learn_rate = 0.05
decay_rate = 0.1
clip_limit = 1.0
tiny_eps = 1e-08
norm_eps = 1e-06

MESH = pl.DeviceIdType.MESH
F32 = jnp.float32
CHUNKS = 4
BLOCK = 2048


def adam_update(gradient, master, first, second, clip_factor):
    scaled = clip_factor * gradient
    new_first = beta_first * first + (1.0 - beta_first) * scaled
    new_second = beta_second * second + (1.0 - beta_second) * scaled * scaled
    direction = new_first / correct_first / (jnp.sqrt(new_second / correct_second) + tiny_eps)
    new_master = master - learn_rate * (decay_rate * master + direction)
    return (new_master, new_first, new_second)


def kernel(
    Z, X, E, share,
    grads, master_in, first_in, second_in,
    params_out, master_out, first_out, second_out,
    own, xr, low, high, sbuf, master, first, second, gathered, norms, norms2,
    own_sem, state_sem, out_sem, x_send, x_recv, z_send, low_recv, high_recv,
    n_send, n_recv, m_send, m_recv, g_send, g_recv, p_sem,
):
    n = Z * X
    dp = lax.axis_index("dp")
    ex = lax.axis_index("expert")
    z, x = dp // X, dp % X
    chunk = share // CHUNKS

    def at_dp(zz, xx):
        return (zz * X + xx, ex)

    def lanes(base, size):
        return pl.ds(pl.multiple_of(base, 128), size)

    barrier = pltpu.get_barrier_semaphore()
    for k in range(1, n):
        pl.semaphore_signal(barrier, inc=1, device_id=((dp + k) % n, ex), device_id_type=MESH)
    for k in range(1, E):
        pl.semaphore_signal(barrier, inc=1, device_id=(dp, (ex + k) % E), device_id_type=MESH)
    pl.semaphore_wait(barrier, n - 1 + E - 1)

    def own_copy(zz):
        return pltpu.make_async_copy(
            grads.at[:, lanes((zz * X + x) * share, share)], own.at[zz], own_sem.at[zz]
        )

    def x_copy(zz, k, c):
        to = (x + k) % X
        return pltpu.make_async_remote_copy(
            src_ref=grads.at[:, lanes((zz * X + to) * share + c * chunk, chunk)],
            dst_ref=xr.at[zz, k - 1, :, lanes(c * chunk, chunk)],
            send_sem=x_send.at[zz, k - 1, c],
            recv_sem=x_recv.at[zz, k - 1, c],
            device_id=at_dp(z, to),
            device_id_type=MESH,
        )

    def for_dest(k, act):
        @pl.when(z + k < Z)
        def _():
            act(z + k)

        if k:
            @pl.when(z - k >= 0)
            def _():
                act(z - k)

    def start_first(zz):
        own_copy(zz).start()

        def body(c, carry):
            for k in range(1, X):
                x_copy(zz, k, c).start()
            return carry

        lax.fori_loop(0, CHUNKS, body, 0)

    for k in range(Z - 1, -1, -1):
        for_dest(k, start_first)
    states = [
        pltpu.make_async_copy(a, b, state_sem.at[i])
        for i, (a, b) in enumerate(((master_in, master), (first_in, first), (second_in, second)))
    ]
    for s in states:
        s.start()

    def z_copy(zz, c, up):
        where = lanes(c * chunk, chunk)
        return pltpu.make_async_remote_copy(
            src_ref=sbuf.at[zz, :, where],
            dst_ref=(low if up else high).at[zz, :, where],
            send_sem=z_send.at[zz, c],
            recv_sem=(low_recv if up else high_recv).at[zz, c],
            device_id=at_dp(z + 1 if up else z - 1, x),
            device_id_type=MESH,
        )

    def sum_block(zz, where, extras):
        total = own[zz, :, where].astype(F32)
        for k in range(1, X):
            total = total + xr[zz, k - 1, :, where].astype(F32)
        for r in extras:
            total = total + r[zz, :, where]
        return total

    def add_chunk(zz, c, extras):
        def body(b, carry):
            where = lanes(c * chunk + b * BLOCK, BLOCK)
            sbuf[zz, :, where] = sum_block(zz, where, extras)
            return carry

        lax.fori_loop(0, chunk // BLOCK, body, 0)

    def hop(zz, c, up):
        for k in range(1, X):
            x_copy(zz, k, c).wait_recv()
        edge = z == (0 if up else Z - 1)

        @pl.when(edge)
        def _():
            add_chunk(zz, c, ())

        @pl.when(jnp.logical_not(edge))
        def _():
            z_copy(zz, c, up).wait_recv()
            add_chunk(zz, c, (low if up else high,))

        z_copy(zz, c, up).start()

    for k in range(Z - 1, 0, -1):
        for_dest(k, lambda zz: own_copy(zz).wait())

        def body(c, carry, k=k):
            @pl.when(z + k < Z)
            def _():
                hop(z + k, c, True)

            @pl.when(z - k >= 0)
            def _():
                hop(z - k, c, False)

            return carry

        lax.fori_loop(0, CHUNKS, body, 0)

    own_copy(z).wait()
    norms2[0] = jnp.zeros((8, 128), F32)

    def finish_chunk(c, extras):
        def body(b, carry):
            where = lanes(c * chunk + b * BLOCK, BLOCK)
            mean = sum_block(z, where, extras) / n
            sbuf[z, :, where] = mean
            return carry + mean * mean

        squares = lax.fori_loop(0, chunk // BLOCK, body, jnp.zeros((own.shape[1], BLOCK), F32))
        norms2[0] = norms2[0] + jnp.full((8, 128), jnp.sum(squares), F32)

    def finish(c, carry):
        for k in range(1, X):
            x_copy(z, k, c).wait_recv()

        @pl.when(z > 0)
        def _():
            z_copy(z, c, True).wait_recv()

        @pl.when(z < Z - 1)
        def _():
            z_copy(z, c, False).wait_recv()

        @pl.when(z == 0)
        def _():
            finish_chunk(c, (high,))

        @pl.when(z == Z - 1)
        def _():
            finish_chunk(c, (low,))

        @pl.when(jnp.logical_and(z > 0, z < Z - 1))
        def _():
            finish_chunk(c, (low, high))

        return carry

    lax.fori_loop(0, CHUNKS, finish, 0)

    norms[0] = norms2[0]

    def n_copy(k):
        return pltpu.make_async_remote_copy(
            src_ref=norms.at[0], dst_ref=norms.at[k],
            send_sem=n_send.at[k], recv_sem=n_recv.at[k],
            device_id=((dp + k) % n, ex), device_id_type=MESH,
        )

    def m_copy(k):
        return pltpu.make_async_remote_copy(
            src_ref=norms2.at[0], dst_ref=norms2.at[k],
            send_sem=m_send.at[k], recv_sem=m_recv.at[k],
            device_id=(dp, (ex + k) % E), device_id_type=MESH,
        )

    for k in range(1, n):
        n_copy(k).start()
    for s in states:
        s.wait()
    total = norms[0]
    for k in range(1, n):
        n_copy(k).wait_recv()
        total = total + norms[k]
    norms2[0] = total
    for k in range(1, E):
        m_copy(k).start()
    for k in range(1, E):
        m_copy(k).wait_recv()
        total = total + norms2[k]
    clip_all = jnp.minimum(1.0, clip_limit / (jnp.sqrt(total) + norm_eps))
    clip_factor = jnp.max(clip_all)

    def g_copy(zz, c, way):
        where = lanes((zz * X + x) * share + c * chunk, chunk)
        if way < 2:
            target = at_dp(z + 1 if way == 0 else z - 1, x)
        else:
            target = at_dp(z, (x + way - 1) % X)
        return pltpu.make_async_remote_copy(
            src_ref=gathered.at[:, where], dst_ref=gathered.at[:, where],
            send_sem=g_send.at[way, zz, c], recv_sem=g_recv.at[zz * X + x, c],
            device_id=target, device_id_type=MESH,
        )

    def arrived(zz, xx, c):
        where = lanes((zz * X + xx) * share + c * chunk, chunk)
        pltpu.make_async_remote_copy(
            src_ref=gathered.at[:, where], dst_ref=gathered.at[:, where],
            send_sem=g_send.at[0, 0, c], recv_sem=g_recv.at[zz * X + xx, c],
            device_id=(dp, (ex + 1) % E), device_id_type=MESH,
        ).wait_recv()

    def put(zz, xx, c):
        where = lanes((zz * X + xx) * share + c * chunk, chunk)
        return pltpu.make_async_copy(
            gathered.at[:, where], params_out.at[:, where], p_sem.at[zz * X + xx, c]
        )

    outs = ((master, master_out), (first, first_out), (second, second_out))

    def out_copy(i, c):
        where = lanes(c * chunk, chunk)
        a, b = outs[i]
        return pltpu.make_async_copy(a.at[:, where], b.at[:, where], out_sem.at[i, c])

    def update(c, carry):
        def body(b, inner):
            where = lanes(c * chunk + b * BLOCK, BLOCK)
            m, f, s = adam_update(
                sbuf[z, :, where], master[:, where], first[:, where], second[:, where], clip_factor
            )
            master[:, where] = m
            first[:, where] = f
            second[:, where] = s
            gathered[:, lanes(dp * share + c * chunk + b * BLOCK, BLOCK)] = m.astype(jnp.bfloat16)
            return inner

        lax.fori_loop(0, chunk // BLOCK, body, 0)

        @pl.when(z < Z - 1)
        def _():
            g_copy(z, c, 0).start()

        @pl.when(z > 0)
        def _():
            g_copy(z, c, 1).start()

        for k in range(1, X):
            g_copy(z, c, k + 1).start()
        for i in range(3):
            out_copy(i, c).start()
        put(z, x, c).start()
        return carry

    lax.fori_loop(0, CHUNKS, update, 0)

    for s in range(1, Z):
        def relay(c, carry, s=s):
            @pl.when(z - s >= 0)
            def _():
                arrived(z - s, x, c)

                @pl.when(z < Z - 1)
                def _():
                    g_copy(z - s, c, 0).start()

                for k in range(1, X):
                    g_copy(z - s, c, k + 1).start()
                put(z - s, x, c).start()

            @pl.when(z + s < Z)
            def _():
                arrived(z + s, x, c)

                @pl.when(z > 0)
                def _():
                    g_copy(z + s, c, 1).start()

                for k in range(1, X):
                    g_copy(z + s, c, k + 1).start()
                put(z + s, x, c).start()

            return carry

        lax.fori_loop(0, CHUNKS, relay, 0)

    for s in range(Z):
        def collect(zz):
            def body(c, carry):
                for k in range(1, X):
                    arrived(zz, (x + k) % X, c)
                    put(zz, (x + k) % X, c).start()
                return carry

            lax.fori_loop(0, CHUNKS, body, 0)

        for_dest(s, collect)

    def drain(c, carry):
        for zz in range(Z):
            for k in range(1, X):
                x_copy(zz, k, c).wait_send()
                g_copy(zz, c, k + 1).wait_send()

            @pl.when(zz > z)
            def _():
                z_copy(zz, c, True).wait_send()

            @pl.when(zz < z)
            def _():
                z_copy(zz, c, False).wait_send()

            @pl.when(jnp.logical_and(zz <= z, z < Z - 1))
            def _():
                g_copy(zz, c, 0).wait_send()

            @pl.when(jnp.logical_and(zz >= z, z > 0))
            def _():
                g_copy(zz, c, 1).wait_send()

            for xx in range(X):
                put(zz, xx, c).wait()
        for i in range(3):
            out_copy(i, c).wait()
        return carry

    lax.fori_loop(0, CHUNKS, drain, 0)
    for k in range(1, n):
        n_copy(k).wait_send()
    for k in range(1, E):
        m_copy(k).wait_send()


def split(count):
    rows = 1
    while rows * rows < count:
        rows *= 2
    return rows, count // rows


def shards(Z, X, E, local_grads, master_weights, first_moment, second_moment):
    layers, flat = local_grads.shape[2:]
    n = Z * X
    share = flat // n
    whole = pl.BlockSpec(memory_space=pl.ANY)
    piece = jax.ShapeDtypeStruct((layers, share), F32)
    dma = pltpu.SemaphoreType.DMA
    state = pltpu.VMEM((layers, share), F32)
    results = pl.pallas_call(
        functools.partial(kernel, Z, X, E, share),
        out_shape=(jax.ShapeDtypeStruct((layers, flat), jnp.bfloat16), piece, piece, piece),
        in_specs=[whole] * 4,
        out_specs=(whole,) * 4,
        scratch_shapes=[
            pltpu.VMEM((Z, layers, share), jnp.bfloat16),
            pltpu.VMEM((Z, X - 1, layers, share), jnp.bfloat16),
            pltpu.VMEM((Z, layers, share), F32),
            pltpu.VMEM((Z, layers, share), F32),
            pltpu.VMEM((Z, layers, share), F32),
            state, state, state,
            pltpu.VMEM((layers, flat), jnp.bfloat16),
            pltpu.VMEM((n, 8, 128), F32),
            pltpu.VMEM((E, 8, 128), F32),
            dma((Z,)), dma((3,)), dma((3, CHUNKS)),
            dma((Z, X - 1, CHUNKS)), dma((Z, X - 1, CHUNKS)),
            dma((Z, CHUNKS)), dma((Z, CHUNKS)), dma((Z, CHUNKS)),
            dma((n,)), dma((n,)), dma((E,)), dma((E,)),
            dma((X + 1, Z, CHUNKS)), dma((n, CHUNKS)), dma((n, CHUNKS)),
        ],
        compiler_params=pltpu.CompilerParams(
            collective_id=0, has_side_effects=True, vmem_limit_bytes=60 * 1024 * 1024
        ),
    )(local_grads[0, 0], master_weights[0], first_moment[0], second_moment[0])
    return tuple(r[None] for r in results)


def solution(mesh):
    Z, X = split(mesh.shape["dp"])
    moments = P("expert", None, "dp")
    return jax.shard_map(
        functools.partial(shards, Z, X, mesh.shape["expert"]),
        mesh=mesh,
        in_specs=(P("dp", "expert", None, None), moments, moments, moments),
        out_specs=(P("expert", None, None), moments, moments, moments),
        check_vma=False,
    )
```

```python
import functools

import jax
import jax.numpy as jnp
from jax import lax
from jax.experimental import pallas as pl
from jax.experimental.pallas import tpu as pltpu
from jax.sharding import PartitionSpec as P

beta_first = 0.9
beta_second = 0.95
correct_first = 1.0 - 0.9**10
correct_second = 1.0 - 0.95**10
learn_rate = 0.05
decay_rate = 0.1
clip_limit = 1.0
tiny_eps = 1e-08
norm_eps = 1e-06

MESH = pl.DeviceIdType.MESH
F32 = jnp.float32
CHUNKS = 8
HALF = CHUNKS // 2
PIECES = 8
SPARE_BYTES = 4 * 1024 * 1024
BLOCK = 2048


def adam_update(gradient, master, first, second, clip_factor):
    scaled = clip_factor * gradient
    new_first = beta_first * first + (1.0 - beta_first) * scaled
    new_second = beta_second * second + (1.0 - beta_second) * scaled * scaled
    direction = new_first / correct_first / (jnp.sqrt(new_second / correct_second) + tiny_eps)
    new_master = master - learn_rate * (decay_rate * master + direction)
    return (new_master, new_first, new_second)


def kernel(
    Z, X, E, share,
    grads, master_in, first_in, second_in,
    gathered, master, first, second,
    xr, low, high, sbuf, norms, norms2,
    x_send, x_recv, z_send, low_recv, high_recv,
    n_send, n_recv, m_send, m_recv, g_send, g_recv, h_send,
):
    n = Z * X
    dp = lax.axis_index("dp")
    ex = lax.axis_index("expert")
    z, x = dp // X, dp % X
    chunk = share // CHUNKS

    def at_dp(zz, xx):
        return (zz * X + xx, ex)

    def lanes(base, size):
        return pl.ds(pl.multiple_of(base, 128), size)

    barrier = pltpu.get_barrier_semaphore()
    for k in range(1, n):
        pl.semaphore_signal(barrier, inc=1, device_id=((dp + k) % n, ex), device_id_type=MESH)
    for k in range(1, E):
        pl.semaphore_signal(barrier, inc=1, device_id=(dp, (ex + k) % E), device_id_type=MESH)
    pl.semaphore_wait(barrier, n - 1 + E - 1)

    def x_copy(zz, k, c):
        to = (x + k) % X
        return pltpu.make_async_remote_copy(
            src_ref=grads.at[:, lanes((zz * X + to) * share + c * chunk, chunk)],
            dst_ref=xr.at[zz, k - 1, :, lanes(c * chunk, chunk)],
            send_sem=x_send.at[zz, k - 1, c],
            recv_sem=x_recv.at[zz, k - 1, c],
            device_id=at_dp(z, to),
            device_id_type=MESH,
        )

    def for_dest(k, act):
        @pl.when(z + k < Z)
        def _():
            act(z + k)

        if k:
            @pl.when(z - k >= 0)
            def _():
                act(z - k)

    def start_first(zz):
        def body(c, carry):
            for k in range(1, X):
                x_copy(zz, k, c).start()
            return carry

        lax.fori_loop(0, CHUNKS, body, 0)

    for k in range(Z - 1, -1, -1):
        for_dest(k, start_first)
    def z_copy(zz, c, up):
        where = lanes(c * chunk, chunk)
        return pltpu.make_async_remote_copy(
            src_ref=sbuf.at[zz, :, where],
            dst_ref=(low if up else high).at[zz, :, where],
            send_sem=z_send.at[zz, c],
            recv_sem=(low_recv if up else high_recv).at[zz, c],
            device_id=at_dp(z + 1 if up else z - 1, x),
            device_id_type=MESH,
        )

    def sum_block(zz, at, extras):
        where = lanes(at, BLOCK)
        total = grads[:, lanes((zz * X + x) * share + at, BLOCK)].astype(F32)
        for k in range(1, X):
            total = total + xr[zz, k - 1, :, where].astype(F32)
        for r in extras:
            total = total + r[zz, :, where]
        return total

    def add_chunk(zz, c, extras):
        def body(b, carry):
            at = c * chunk + b * BLOCK
            sbuf[zz, :, lanes(at, BLOCK)] = sum_block(zz, at, extras)
            return carry

        lax.fori_loop(0, chunk // BLOCK, body, 0)

    def hop(zz, c, up):
        for k in range(1, X):
            x_copy(zz, k, c).wait_recv()
        edge = z == (0 if up else Z - 1)

        @pl.when(edge)
        def _():
            add_chunk(zz, c, ())

        @pl.when(jnp.logical_not(edge))
        def _():
            z_copy(zz, c, up).wait_recv()
            add_chunk(zz, c, (low if up else high,))

        z_copy(zz, c, up).start()

    for k in range(Z - 1, 0, -1):
        def body(c, carry, k=k):
            @pl.when(z + k < Z)
            def _():
                hop(z + k, c, True)

            @pl.when(z - k >= 0)
            def _():
                hop(z - k, c, False)

            return carry

        lax.fori_loop(0, CHUNKS, body, 0)

    norms2[0] = jnp.zeros((8, 128), F32)

    def finish_chunk(c, extras):
        def body(b, carry):
            at = c * chunk + b * BLOCK
            mean = sum_block(z, at, extras) / n
            sbuf[z, :, lanes(at, BLOCK)] = mean
            return carry + mean * mean

        squares = lax.fori_loop(0, chunk // BLOCK, body, jnp.zeros((grads.shape[0], BLOCK), F32))
        norms2[0] = norms2[0] + jnp.full((8, 128), jnp.sum(squares), F32)

    def finish(c, carry):
        for k in range(1, X):
            x_copy(z, k, c).wait_recv()

        @pl.when(z > 0)
        def _():
            z_copy(z, c, True).wait_recv()

        @pl.when(z < Z - 1)
        def _():
            z_copy(z, c, False).wait_recv()

        @pl.when(z == 0)
        def _():
            finish_chunk(c, (high,))

        @pl.when(z == Z - 1)
        def _():
            finish_chunk(c, (low,))

        @pl.when(jnp.logical_and(z > 0, z < Z - 1))
        def _():
            finish_chunk(c, (low, high))

        return carry

    lax.fori_loop(0, CHUNKS, finish, 0)

    norms[0] = norms2[0]

    def n_copy(k):
        return pltpu.make_async_remote_copy(
            src_ref=norms.at[0], dst_ref=norms.at[k],
            send_sem=n_send.at[k], recv_sem=n_recv.at[k],
            device_id=((dp + k) % n, ex), device_id_type=MESH,
        )

    def m_copy(k):
        return pltpu.make_async_remote_copy(
            src_ref=norms2.at[0], dst_ref=norms2.at[k],
            send_sem=m_send.at[k], recv_sem=m_recv.at[k],
            device_id=(dp, (ex + k) % E), device_id_type=MESH,
        )

    for k in range(1, n):
        n_copy(k).start()
    total = norms[0]
    for k in range(1, n):
        n_copy(k).wait_recv()
        total = total + norms[k]
    norms2[0] = total
    for k in range(1, E):
        m_copy(k).start()
    for k in range(1, E):
        m_copy(k).wait_recv()
        total = total + norms2[k]
    clip_all = jnp.minimum(1.0, clip_limit / (jnp.sqrt(total) + norm_eps))
    clip_factor = jnp.max(clip_all)

    def g_copy(zz, c, way):
        where = lanes((zz * X + x) * share + c * chunk, chunk)
        if way < 2:
            target = at_dp(z + 1 if way == 0 else z - 1, x)
        else:
            target = at_dp(z, (x + way - 1) % X)
        return pltpu.make_async_remote_copy(
            src_ref=gathered.at[:, where], dst_ref=gathered.at[:, where],
            send_sem=g_send.at[way, zz, c], recv_sem=g_recv.at[zz * X + x, c],
            device_id=target, device_id_type=MESH,
        )

    def arrived(zz, xx, c):
        where = lanes((zz * X + xx) * share + c * chunk, chunk)
        pltpu.make_async_remote_copy(
            src_ref=gathered.at[:, where], dst_ref=gathered.at[:, where],
            send_sem=g_send.at[0, 0, c], recv_sem=g_recv.at[zz * X + xx, c],
            device_id=(dp, (ex + 1) % E), device_id_type=MESH,
        ).wait_recv()

    pair = z + 1 - 2 * (z % 2)

    def h_copy(k, c):
        where = lanes((z * X + (x + k) % X) * share + c * chunk, chunk)
        return pltpu.make_async_remote_copy(
            src_ref=gathered.at[:, where], dst_ref=gathered.at[:, where],
            send_sem=h_send.at[k - 1, c], recv_sem=g_recv.at[z * X + (x + k) % X, c],
            device_id=at_dp(pair, x), device_id_type=MESH,
        )

    def along_x(zz, c, act):
        @pl.when(jnp.logical_or(zz != pair, c < HALF))
        def _():
            for k in range(1, X):
                act(g_copy(zz, c, k + 1))

    def update(c, carry):
        def body(b, inner):
            where = lanes(c * chunk + b * BLOCK, BLOCK)
            m, f, s = adam_update(
                sbuf[z, :, where], master_in[:, where], first_in[:, where], second_in[:, where], clip_factor
            )
            master[:, where] = m
            first[:, where] = f
            second[:, where] = s
            gathered[:, lanes(dp * share + c * chunk + b * BLOCK, BLOCK)] = m.astype(jnp.bfloat16)
            return inner

        lax.fori_loop(0, chunk // BLOCK, body, 0)

        @pl.when(z < Z - 1)
        def _():
            g_copy(z, c, 0).start()

        @pl.when(z > 0)
        def _():
            g_copy(z, c, 1).start()

        for k in range(1, X):
            g_copy(z, c, k + 1).start()
        return carry

    lax.fori_loop(0, CHUNKS, update, 0)

    for s in range(1, Z):
        def relay(c, carry, s=s):
            @pl.when(z - s >= 0)
            def _():
                arrived(z - s, x, c)

                @pl.when(z < Z - 1)
                def _():
                    g_copy(z - s, c, 0).start()

                along_x(z - s, c, lambda copy: copy.start())

            @pl.when(z + s < Z)
            def _():
                arrived(z + s, x, c)

                @pl.when(z > 0)
                def _():
                    g_copy(z + s, c, 1).start()

                along_x(z + s, c, lambda copy: copy.start())

            return carry

        lax.fori_loop(0, CHUNKS, relay, 0)

        if s == 1:
            def across(c, carry):
                for k in range(1, X):
                    arrived(z, (x + k) % X, c)
                    h_copy(k, c).start()
                return carry

            lax.fori_loop(HALF, CHUNKS, across, 0)

    for s in range(Z):
        def collect(zz, s=s):
            def body(c, carry):
                for k in range(1, X):
                    arrived(zz, (x + k) % X, c)
                return carry

            lax.fori_loop(0, HALF if s == 0 else CHUNKS, body, 0)

        for_dest(s, collect)

    def drain(c, carry):
        for zz in range(Z):
            for k in range(1, X):
                x_copy(zz, k, c).wait_send()
            along_x(zz, c, lambda copy: copy.wait_send())

            @pl.when(zz > z)
            def _():
                z_copy(zz, c, True).wait_send()

            @pl.when(zz < z)
            def _():
                z_copy(zz, c, False).wait_send()

            @pl.when(jnp.logical_and(zz <= z, z < Z - 1))
            def _():
                g_copy(zz, c, 0).wait_send()

            @pl.when(jnp.logical_and(zz >= z, z > 0))
            def _():
                g_copy(zz, c, 1).wait_send()

        @pl.when(c >= HALF)
        def _():
            for k in range(1, X):
                h_copy(k, c).wait_send()

        return carry

    lax.fori_loop(0, CHUNKS, drain, 0)
    for k in range(1, n):
        n_copy(k).wait_send()
    for k in range(1, E):
        m_copy(k).wait_send()


def write_out(count, *refs):
    sources, targets, sem = refs[:count], refs[count : 2 * count], refs[2 * count]

    def copies(i):
        size = sources[i].shape[1] // PIECES
        for p in range(PIECES):
            where = pl.ds(p * size, size)
            yield pltpu.make_async_copy(sources[i].at[:, where], targets[i].at[:, where], sem.at[i, p])

    for i in range(count):
        for copy in copies(i):
            copy.start()
    for i in range(count):
        for copy in copies(i):
            copy.wait()


def split(count):
    rows = 1
    while rows * rows < count:
        rows *= 2
    return rows, count // rows


def shards(Z, X, E, local_grads, master_weights, first_moment, second_moment):
    layers, flat = local_grads.shape[2:]
    n = Z * X
    share = flat // n
    whole = pl.BlockSpec(memory_space=pltpu.HBM)
    piece = jax.ShapeDtypeStruct((layers, share), F32)
    dma = pltpu.SemaphoreType.DMA
    local = pl.BlockSpec(memory_space=pltpu.VMEM)
    shapes = (jax.ShapeDtypeStruct((layers, flat), jnp.bfloat16), piece, piece, piece)
    out_bytes = layers * (2 * flat + 3 * 4 * share)
    used_bytes = layers * Z * share * (2 * X + 3 * 4) + 2 * out_bytes
    results = pl.pallas_call(
        functools.partial(kernel, Z, X, E, share),
        out_shape=shapes,
        in_specs=[local] * 4,
        out_specs=(local,) * 4,
        scratch_shapes=[
            pltpu.VMEM((Z, X - 1, layers, share), jnp.bfloat16),
            pltpu.VMEM((Z, layers, share), F32),
            pltpu.VMEM((Z, layers, share), F32),
            pltpu.VMEM((Z, layers, share), F32),
            pltpu.VMEM((n, 8, 128), F32),
            pltpu.VMEM((E, 8, 128), F32),
            dma((Z, X - 1, CHUNKS)), dma((Z, X - 1, CHUNKS)),
            dma((Z, CHUNKS)), dma((Z, CHUNKS)), dma((Z, CHUNKS)),
            dma((n,)), dma((n,)), dma((E,)), dma((E,)),
            dma((X + 1, Z, CHUNKS)), dma((n, CHUNKS)), dma((X - 1, CHUNKS)),
        ],
        compiler_params=pltpu.CompilerParams(
            collective_id=0, has_side_effects=True, vmem_limit_bytes=used_bytes + SPARE_BYTES
        ),
    )(local_grads[0, 0], master_weights[0], first_moment[0], second_moment[0])
    results = pl.pallas_call(
        functools.partial(write_out, len(shapes)),
        out_shape=shapes,
        in_specs=[local] * 4,
        out_specs=(whole,) * 4,
        scratch_shapes=[dma((len(shapes), PIECES))],
        compiler_params=pltpu.CompilerParams(vmem_limit_bytes=out_bytes + SPARE_BYTES),
    )(*results)
    return tuple(r[None] for r in results)


def solution(mesh):
    Z, X = split(mesh.shape["dp"])
    moments = P("expert", None, "dp")
    return jax.shard_map(
        functools.partial(shards, Z, X, mesh.shape["expert"]),
        mesh=mesh,
        in_specs=(P("dp", "expert", None, None), moments, moments, moments),
        out_specs=(P("expert", None, None), moments, moments, moments),
        check_vma=False,
    )
```

```python
import functools

import jax
import jax.numpy as jnp
from jax import lax
from jax.experimental import pallas as pl
from jax.experimental.pallas import tpu as pltpu
from jax.sharding import PartitionSpec as P

beta_first = 0.9
beta_second = 0.95
correct_first = 1.0 - 0.9**10
correct_second = 1.0 - 0.95**10
learn_rate = 0.05
decay_rate = 0.1
clip_limit = 1.0
tiny_eps = 1e-08
norm_eps = 1e-06

MESH = pl.DeviceIdType.MESH
F32 = jnp.float32
CHUNKS = 8
HALF = CHUNKS // 2
PIECES = 8
SPARE_BYTES = 4 * 1024 * 1024
BLOCK = 2048


def adam_update(gradient, master, first, second, clip_factor):
    scaled = clip_factor * gradient
    new_first = beta_first * first + (1.0 - beta_first) * scaled
    new_second = beta_second * second + (1.0 - beta_second) * scaled * scaled
    direction = new_first / correct_first / (jnp.sqrt(new_second / correct_second) + tiny_eps)
    new_master = master - learn_rate * (decay_rate * master + direction)
    return (new_master, new_first, new_second)


def kernel(
    Z, X, E, share,
    grads, master_in, first_in, second_in,
    gathered, master, first, second,
    own, xr, low, high, sbuf, norms, norms2,
    own_sem, state_sem, x_send, x_recv, z_send, low_recv, high_recv,
    n_send, n_recv, m_send, m_recv, g_send, g_recv, h_send,
):
    n = Z * X
    dp = lax.axis_index("dp")
    ex = lax.axis_index("expert")
    z, x = dp // X, dp % X
    chunk = share // CHUNKS

    def at_dp(zz, xx):
        return (zz * X + xx, ex)

    def lanes(base, size):
        return pl.ds(pl.multiple_of(base, 128), size)

    barrier = pltpu.get_barrier_semaphore()
    for k in range(1, n):
        pl.semaphore_signal(barrier, inc=1, device_id=((dp + k) % n, ex), device_id_type=MESH)
    for k in range(1, E):
        pl.semaphore_signal(barrier, inc=1, device_id=(dp, (ex + k) % E), device_id_type=MESH)
    pl.semaphore_wait(barrier, n - 1 + E - 1)

    def own_copy(zz):
        return pltpu.make_async_copy(
            grads.at[:, lanes((zz * X + x) * share, share)], own.at[zz], own_sem.at[zz]
        )

    def x_copy(zz, k, c):
        to = (x + k) % X
        return pltpu.make_async_remote_copy(
            src_ref=grads.at[:, lanes((zz * X + to) * share + c * chunk, chunk)],
            dst_ref=xr.at[zz, k - 1, :, lanes(c * chunk, chunk)],
            send_sem=x_send.at[zz, k - 1, c],
            recv_sem=x_recv.at[zz, k - 1, c],
            device_id=at_dp(z, to),
            device_id_type=MESH,
        )

    def for_dest(k, act):
        @pl.when(z + k < Z)
        def _():
            act(z + k)

        if k:
            @pl.when(z - k >= 0)
            def _():
                act(z - k)

    def start_first(zz):
        own_copy(zz).start()

        def body(c, carry):
            for k in range(1, X):
                x_copy(zz, k, c).start()
            return carry

        lax.fori_loop(0, CHUNKS, body, 0)

    for k in range(Z - 1, -1, -1):
        for_dest(k, start_first)
    states = [
        pltpu.make_async_copy(a, b, state_sem.at[i])
        for i, (a, b) in enumerate(((master_in, master), (first_in, first), (second_in, second)))
    ]
    for s in states:
        s.start()

    def z_copy(zz, c, up):
        where = lanes(c * chunk, chunk)
        return pltpu.make_async_remote_copy(
            src_ref=sbuf.at[zz, :, where],
            dst_ref=(low if up else high).at[zz, :, where],
            send_sem=z_send.at[zz, c],
            recv_sem=(low_recv if up else high_recv).at[zz, c],
            device_id=at_dp(z + 1 if up else z - 1, x),
            device_id_type=MESH,
        )

    def sum_block(zz, where, extras):
        total = own[zz, :, where].astype(F32)
        for k in range(1, X):
            total = total + xr[zz, k - 1, :, where].astype(F32)
        for r in extras:
            total = total + r[zz, :, where]
        return total

    def add_chunk(zz, c, extras):
        def body(b, carry):
            where = lanes(c * chunk + b * BLOCK, BLOCK)
            sbuf[zz, :, where] = sum_block(zz, where, extras)
            return carry

        lax.fori_loop(0, chunk // BLOCK, body, 0)

    def hop(zz, c, up):
        for k in range(1, X):
            x_copy(zz, k, c).wait_recv()
        edge = z == (0 if up else Z - 1)

        @pl.when(edge)
        def _():
            add_chunk(zz, c, ())

        @pl.when(jnp.logical_not(edge))
        def _():
            z_copy(zz, c, up).wait_recv()
            add_chunk(zz, c, (low if up else high,))

        z_copy(zz, c, up).start()

    for k in range(Z - 1, 0, -1):
        for_dest(k, lambda zz: own_copy(zz).wait())

        def body(c, carry, k=k):
            @pl.when(z + k < Z)
            def _():
                hop(z + k, c, True)

            @pl.when(z - k >= 0)
            def _():
                hop(z - k, c, False)

            return carry

        lax.fori_loop(0, CHUNKS, body, 0)

    own_copy(z).wait()
    norms2[0] = jnp.zeros((8, 128), F32)

    def finish_chunk(c, extras):
        def body(b, carry):
            where = lanes(c * chunk + b * BLOCK, BLOCK)
            mean = sum_block(z, where, extras) / n
            sbuf[z, :, where] = mean
            return carry + mean * mean

        squares = lax.fori_loop(0, chunk // BLOCK, body, jnp.zeros((own.shape[1], BLOCK), F32))
        norms2[0] = norms2[0] + jnp.full((8, 128), jnp.sum(squares), F32)

    def finish(c, carry):
        for k in range(1, X):
            x_copy(z, k, c).wait_recv()

        @pl.when(z > 0)
        def _():
            z_copy(z, c, True).wait_recv()

        @pl.when(z < Z - 1)
        def _():
            z_copy(z, c, False).wait_recv()

        @pl.when(z == 0)
        def _():
            finish_chunk(c, (high,))

        @pl.when(z == Z - 1)
        def _():
            finish_chunk(c, (low,))

        @pl.when(jnp.logical_and(z > 0, z < Z - 1))
        def _():
            finish_chunk(c, (low, high))

        return carry

    lax.fori_loop(0, CHUNKS, finish, 0)

    norms[0] = norms2[0]

    def n_copy(k):
        return pltpu.make_async_remote_copy(
            src_ref=norms.at[0], dst_ref=norms.at[k],
            send_sem=n_send.at[k], recv_sem=n_recv.at[k],
            device_id=((dp + k) % n, ex), device_id_type=MESH,
        )

    def m_copy(k):
        return pltpu.make_async_remote_copy(
            src_ref=norms2.at[0], dst_ref=norms2.at[k],
            send_sem=m_send.at[k], recv_sem=m_recv.at[k],
            device_id=(dp, (ex + k) % E), device_id_type=MESH,
        )

    for k in range(1, n):
        n_copy(k).start()
    for s in states:
        s.wait()
    total = norms[0]
    for k in range(1, n):
        n_copy(k).wait_recv()
        total = total + norms[k]
    norms2[0] = total
    for k in range(1, E):
        m_copy(k).start()
    for k in range(1, E):
        m_copy(k).wait_recv()
        total = total + norms2[k]
    clip_all = jnp.minimum(1.0, clip_limit / (jnp.sqrt(total) + norm_eps))
    clip_factor = jnp.max(clip_all)

    def g_copy(zz, c, way):
        where = lanes((zz * X + x) * share + c * chunk, chunk)
        if way < 2:
            target = at_dp(z + 1 if way == 0 else z - 1, x)
        else:
            target = at_dp(z, (x + way - 1) % X)
        return pltpu.make_async_remote_copy(
            src_ref=gathered.at[:, where], dst_ref=gathered.at[:, where],
            send_sem=g_send.at[way, zz, c], recv_sem=g_recv.at[zz * X + x, c],
            device_id=target, device_id_type=MESH,
        )

    def arrived(zz, xx, c):
        where = lanes((zz * X + xx) * share + c * chunk, chunk)
        pltpu.make_async_remote_copy(
            src_ref=gathered.at[:, where], dst_ref=gathered.at[:, where],
            send_sem=g_send.at[0, 0, c], recv_sem=g_recv.at[zz * X + xx, c],
            device_id=(dp, (ex + 1) % E), device_id_type=MESH,
        ).wait_recv()

    pair = z + 1 - 2 * (z % 2)

    def h_copy(k, c):
        where = lanes((z * X + (x + k) % X) * share + c * chunk, chunk)
        return pltpu.make_async_remote_copy(
            src_ref=gathered.at[:, where], dst_ref=gathered.at[:, where],
            send_sem=h_send.at[k - 1, c], recv_sem=g_recv.at[z * X + (x + k) % X, c],
            device_id=at_dp(pair, x), device_id_type=MESH,
        )

    def along_x(zz, c, act):
        @pl.when(jnp.logical_or(zz != pair, c < HALF))
        def _():
            for k in range(1, X):
                act(g_copy(zz, c, k + 1))

    def update(c, carry):
        def body(b, inner):
            where = lanes(c * chunk + b * BLOCK, BLOCK)
            m, f, s = adam_update(
                sbuf[z, :, where], master[:, where], first[:, where], second[:, where], clip_factor
            )
            master[:, where] = m
            first[:, where] = f
            second[:, where] = s
            gathered[:, lanes(dp * share + c * chunk + b * BLOCK, BLOCK)] = m.astype(jnp.bfloat16)
            return inner

        lax.fori_loop(0, chunk // BLOCK, body, 0)

        @pl.when(z < Z - 1)
        def _():
            g_copy(z, c, 0).start()

        @pl.when(z > 0)
        def _():
            g_copy(z, c, 1).start()

        for k in range(1, X):
            g_copy(z, c, k + 1).start()
        return carry

    lax.fori_loop(0, CHUNKS, update, 0)

    for s in range(1, Z):
        def relay(c, carry, s=s):
            @pl.when(z - s >= 0)
            def _():
                arrived(z - s, x, c)

                @pl.when(z < Z - 1)
                def _():
                    g_copy(z - s, c, 0).start()

                along_x(z - s, c, lambda copy: copy.start())

            @pl.when(z + s < Z)
            def _():
                arrived(z + s, x, c)

                @pl.when(z > 0)
                def _():
                    g_copy(z + s, c, 1).start()

                along_x(z + s, c, lambda copy: copy.start())

            return carry

        lax.fori_loop(0, CHUNKS, relay, 0)

        if s == 1:
            def across(c, carry):
                for k in range(1, X):
                    arrived(z, (x + k) % X, c)
                    h_copy(k, c).start()
                return carry

            lax.fori_loop(HALF, CHUNKS, across, 0)

    for s in range(Z):
        def collect(zz, s=s):
            def body(c, carry):
                for k in range(1, X):
                    arrived(zz, (x + k) % X, c)
                return carry

            lax.fori_loop(0, HALF if s == 0 else CHUNKS, body, 0)

        for_dest(s, collect)

    def drain(c, carry):
        for zz in range(Z):
            for k in range(1, X):
                x_copy(zz, k, c).wait_send()
            along_x(zz, c, lambda copy: copy.wait_send())

            @pl.when(zz > z)
            def _():
                z_copy(zz, c, True).wait_send()

            @pl.when(zz < z)
            def _():
                z_copy(zz, c, False).wait_send()

            @pl.when(jnp.logical_and(zz <= z, z < Z - 1))
            def _():
                g_copy(zz, c, 0).wait_send()

            @pl.when(jnp.logical_and(zz >= z, z > 0))
            def _():
                g_copy(zz, c, 1).wait_send()

        @pl.when(c >= HALF)
        def _():
            for k in range(1, X):
                h_copy(k, c).wait_send()

        return carry

    lax.fori_loop(0, CHUNKS, drain, 0)
    for k in range(1, n):
        n_copy(k).wait_send()
    for k in range(1, E):
        m_copy(k).wait_send()


def write_out(count, *refs):
    sources, targets, sem = refs[:count], refs[count : 2 * count], refs[2 * count]

    def copies(i):
        size = sources[i].shape[1] // PIECES
        for p in range(PIECES):
            where = pl.ds(p * size, size)
            yield pltpu.make_async_copy(sources[i].at[:, where], targets[i].at[:, where], sem.at[i, p])

    for i in range(count):
        for copy in copies(i):
            copy.start()
    for i in range(count):
        for copy in copies(i):
            copy.wait()


def split(count):
    rows = 1
    while rows * rows < count:
        rows *= 2
    return rows, count // rows


def shards(Z, X, E, local_grads, master_weights, first_moment, second_moment):
    layers, flat = local_grads.shape[2:]
    n = Z * X
    share = flat // n
    whole = pl.BlockSpec(memory_space=pltpu.HBM)
    piece = jax.ShapeDtypeStruct((layers, share), F32)
    dma = pltpu.SemaphoreType.DMA
    local = pl.BlockSpec(memory_space=pltpu.VMEM)
    shapes = (jax.ShapeDtypeStruct((layers, flat), jnp.bfloat16), piece, piece, piece)
    arrays = (local_grads[0, 0], master_weights[0], first_moment[0], second_moment[0])
    out_bytes = layers * (2 * flat + 3 * 4 * share)
    used_bytes = layers * Z * share * (2 * X + 3 * 4) + out_bytes
    results = pl.pallas_call(
        functools.partial(kernel, Z, X, E, share),
        out_shape=shapes,
        in_specs=[whole] * 4,
        out_specs=(local,) * 4,
        scratch_shapes=[
            pltpu.VMEM((Z, layers, share), jnp.bfloat16),
            pltpu.VMEM((Z, X - 1, layers, share), jnp.bfloat16),
            pltpu.VMEM((Z, layers, share), F32),
            pltpu.VMEM((Z, layers, share), F32),
            pltpu.VMEM((Z, layers, share), F32),
            pltpu.VMEM((n, 8, 128), F32),
            pltpu.VMEM((E, 8, 128), F32),
            dma((Z,)), dma((3,)),
            dma((Z, X - 1, CHUNKS)), dma((Z, X - 1, CHUNKS)),
            dma((Z, CHUNKS)), dma((Z, CHUNKS)), dma((Z, CHUNKS)),
            dma((n,)), dma((n,)), dma((E,)), dma((E,)),
            dma((X + 1, Z, CHUNKS)), dma((n, CHUNKS)), dma((X - 1, CHUNKS)),
        ],
        compiler_params=pltpu.CompilerParams(
            collective_id=0, has_side_effects=True, vmem_limit_bytes=used_bytes + SPARE_BYTES
        ),
    )(*(pltpu.with_memory_space_constraint(a, pltpu.HBM) for a in arrays))
    results = pl.pallas_call(
        functools.partial(write_out, len(shapes)),
        out_shape=shapes,
        in_specs=[local] * 4,
        out_specs=(whole,) * 4,
        scratch_shapes=[dma((len(shapes), PIECES))],
        compiler_params=pltpu.CompilerParams(vmem_limit_bytes=out_bytes + SPARE_BYTES),
    )(*results)
    return tuple(r[None] for r in results)


def solution(mesh):
    Z, X = split(mesh.shape["dp"])
    moments = P("expert", None, "dp")
    return jax.shard_map(
        functools.partial(shards, Z, X, mesh.shape["expert"]),
        mesh=mesh,
        in_specs=(P("dp", "expert", None, None), moments, moments, moments),
        out_specs=(P("expert", None, None), moments, moments, moments),
        check_vma=False,
    )
```

```python
import functools

import jax
import jax.numpy as jnp
from jax import lax
from jax.experimental import pallas as pl
from jax.experimental.pallas import tpu as pltpu
from jax.sharding import PartitionSpec as P

beta_first = 0.9
beta_second = 0.95
correct_first = 1.0 - 0.9**10
correct_second = 1.0 - 0.95**10
learn_rate = 0.05
decay_rate = 0.1
clip_limit = 1.0
tiny_eps = 1e-08
norm_eps = 1e-06

MESH = pl.DeviceIdType.MESH
F32 = jnp.float32
CHUNKS = 16
HALF = CHUNKS // 2
PIECES = 8
SPARE_BYTES = 4 * 1024 * 1024
BLOCK = 2048


def adam_update(gradient, master, first, second, clip_factor):
    scaled = clip_factor * gradient
    new_first = beta_first * first + (1.0 - beta_first) * scaled
    new_second = beta_second * second + (1.0 - beta_second) * scaled * scaled
    direction = new_first / correct_first / (jnp.sqrt(new_second / correct_second) + tiny_eps)
    new_master = master - learn_rate * (decay_rate * master + direction)
    return (new_master, new_first, new_second)


def kernel(
    Z, X, E, share,
    grads, master_in, first_in, second_in,
    gathered, master, first, second,
    own, xr, low, high, sbuf, norms, norms2,
    own_sem, state_sem, x_send, x_recv, z_send, low_recv, high_recv,
    n_send, n_recv, m_send, m_recv, g_send, g_recv, h_send,
):
    n = Z * X
    dp = lax.axis_index("dp")
    ex = lax.axis_index("expert")
    z, x = dp // X, dp % X
    chunk = share // CHUNKS

    def at_dp(zz, xx):
        return (zz * X + xx, ex)

    def lanes(base, size):
        return pl.ds(pl.multiple_of(base, 128), size)

    barrier = pltpu.get_barrier_semaphore()
    for k in range(1, n):
        pl.semaphore_signal(barrier, inc=1, device_id=((dp + k) % n, ex), device_id_type=MESH)
    for k in range(1, E):
        pl.semaphore_signal(barrier, inc=1, device_id=(dp, (ex + k) % E), device_id_type=MESH)
    pl.semaphore_wait(barrier, n - 1 + E - 1)

    def own_copy(zz):
        return pltpu.make_async_copy(
            grads.at[:, lanes((zz * X + x) * share, share)], own.at[zz], own_sem.at[zz]
        )

    def x_copy(zz, k, c):
        to = (x + k) % X
        return pltpu.make_async_remote_copy(
            src_ref=grads.at[:, lanes((zz * X + to) * share + c * chunk, chunk)],
            dst_ref=xr.at[zz, k - 1, :, lanes(c * chunk, chunk)],
            send_sem=x_send.at[zz, k - 1, c],
            recv_sem=x_recv.at[zz, k - 1, c],
            device_id=at_dp(z, to),
            device_id_type=MESH,
        )

    def for_dest(k, act):
        @pl.when(z + k < Z)
        def _():
            act(z + k)

        if k:
            @pl.when(z - k >= 0)
            def _():
                act(z - k)

    def start_first(zz):
        own_copy(zz).start()

        def body(c, carry):
            for k in range(1, X):
                x_copy(zz, k, c).start()
            return carry

        lax.fori_loop(0, CHUNKS, body, 0)

    for k in range(Z - 1, -1, -1):
        for_dest(k, start_first)
    states = [
        pltpu.make_async_copy(a, b, state_sem.at[i])
        for i, (a, b) in enumerate(((master_in, master), (first_in, first), (second_in, second)))
    ]
    for s in states:
        s.start()

    def z_copy(zz, c, up):
        where = lanes(c * chunk, chunk)
        return pltpu.make_async_remote_copy(
            src_ref=sbuf.at[zz, :, where],
            dst_ref=(low if up else high).at[zz, :, where],
            send_sem=z_send.at[zz, c],
            recv_sem=(low_recv if up else high_recv).at[zz, c],
            device_id=at_dp(z + 1 if up else z - 1, x),
            device_id_type=MESH,
        )

    def sum_block(zz, where, extras):
        total = own[zz, :, where].astype(F32)
        for k in range(1, X):
            total = total + xr[zz, k - 1, :, where].astype(F32)
        for r in extras:
            total = total + r[zz, :, where]
        return total

    def add_chunk(zz, c, extras):
        def body(b, carry):
            where = lanes(c * chunk + b * BLOCK, BLOCK)
            sbuf[zz, :, where] = sum_block(zz, where, extras)
            return carry

        lax.fori_loop(0, chunk // BLOCK, body, 0)

    def hop(zz, c, up):
        for k in range(1, X):
            x_copy(zz, k, c).wait_recv()
        edge = z == (0 if up else Z - 1)

        @pl.when(edge)
        def _():
            add_chunk(zz, c, ())

        @pl.when(jnp.logical_not(edge))
        def _():
            z_copy(zz, c, up).wait_recv()
            add_chunk(zz, c, (low if up else high,))

        z_copy(zz, c, up).start()

    for k in range(Z - 1, 0, -1):
        for_dest(k, lambda zz: own_copy(zz).wait())

        def body(c, carry, k=k):
            @pl.when(z + k < Z)
            def _():
                hop(z + k, c, True)

            @pl.when(z - k >= 0)
            def _():
                hop(z - k, c, False)

            return carry

        lax.fori_loop(0, CHUNKS, body, 0)

    own_copy(z).wait()
    norms2[0] = jnp.zeros((8, 128), F32)

    def finish_chunk(c, extras):
        def body(b, carry):
            where = lanes(c * chunk + b * BLOCK, BLOCK)
            mean = sum_block(z, where, extras) / n
            sbuf[z, :, where] = mean
            return carry + mean * mean

        squares = lax.fori_loop(0, chunk // BLOCK, body, jnp.zeros((own.shape[1], BLOCK), F32))
        norms2[0] = norms2[0] + jnp.full((8, 128), jnp.sum(squares), F32)

    def finish(c, carry):
        for k in range(1, X):
            x_copy(z, k, c).wait_recv()

        @pl.when(z > 0)
        def _():
            z_copy(z, c, True).wait_recv()

        @pl.when(z < Z - 1)
        def _():
            z_copy(z, c, False).wait_recv()

        @pl.when(z == 0)
        def _():
            finish_chunk(c, (high,))

        @pl.when(z == Z - 1)
        def _():
            finish_chunk(c, (low,))

        @pl.when(jnp.logical_and(z > 0, z < Z - 1))
        def _():
            finish_chunk(c, (low, high))

        return carry

    lax.fori_loop(0, CHUNKS, finish, 0)

    norms[0] = norms2[0]

    def n_copy(k):
        return pltpu.make_async_remote_copy(
            src_ref=norms.at[0], dst_ref=norms.at[k],
            send_sem=n_send.at[k], recv_sem=n_recv.at[k],
            device_id=((dp + k) % n, ex), device_id_type=MESH,
        )

    def m_copy(k):
        return pltpu.make_async_remote_copy(
            src_ref=norms2.at[0], dst_ref=norms2.at[k],
            send_sem=m_send.at[k], recv_sem=m_recv.at[k],
            device_id=(dp, (ex + k) % E), device_id_type=MESH,
        )

    for k in range(1, n):
        n_copy(k).start()
    for s in states:
        s.wait()
    total = norms[0]
    for k in range(1, n):
        n_copy(k).wait_recv()
        total = total + norms[k]
    norms2[0] = total
    for k in range(1, E):
        m_copy(k).start()
    for k in range(1, E):
        m_copy(k).wait_recv()
        total = total + norms2[k]
    clip_all = jnp.minimum(1.0, clip_limit / (jnp.sqrt(total) + norm_eps))
    clip_factor = jnp.max(clip_all)

    def g_copy(zz, c, way):
        where = lanes((zz * X + x) * share + c * chunk, chunk)
        if way < 2:
            target = at_dp(z + 1 if way == 0 else z - 1, x)
        else:
            target = at_dp(z, (x + way - 1) % X)
        return pltpu.make_async_remote_copy(
            src_ref=gathered.at[:, where], dst_ref=gathered.at[:, where],
            send_sem=g_send.at[way, zz, c], recv_sem=g_recv.at[zz * X + x, c],
            device_id=target, device_id_type=MESH,
        )

    def arrived(zz, xx, c):
        where = lanes((zz * X + xx) * share + c * chunk, chunk)
        pltpu.make_async_remote_copy(
            src_ref=gathered.at[:, where], dst_ref=gathered.at[:, where],
            send_sem=g_send.at[0, 0, c], recv_sem=g_recv.at[zz * X + xx, c],
            device_id=(dp, (ex + 1) % E), device_id_type=MESH,
        ).wait_recv()

    pair = z + 1 - 2 * (z % 2)

    def h_copy(k, c):
        where = lanes((z * X + (x + k) % X) * share + c * chunk, chunk)
        return pltpu.make_async_remote_copy(
            src_ref=gathered.at[:, where], dst_ref=gathered.at[:, where],
            send_sem=h_send.at[k - 1, c], recv_sem=g_recv.at[z * X + (x + k) % X, c],
            device_id=at_dp(pair, x), device_id_type=MESH,
        )

    def along_x(zz, c, act):
        @pl.when(jnp.logical_or(zz != pair, c < HALF))
        def _():
            for k in range(1, X):
                act(g_copy(zz, c, k + 1))

    def update(c, carry):
        def body(b, inner):
            where = lanes(c * chunk + b * BLOCK, BLOCK)
            m, f, s = adam_update(
                sbuf[z, :, where], master[:, where], first[:, where], second[:, where], clip_factor
            )
            master[:, where] = m
            first[:, where] = f
            second[:, where] = s
            gathered[:, lanes(dp * share + c * chunk + b * BLOCK, BLOCK)] = m.astype(jnp.bfloat16)
            return inner

        lax.fori_loop(0, chunk // BLOCK, body, 0)

        @pl.when(z < Z - 1)
        def _():
            g_copy(z, c, 0).start()

        @pl.when(z > 0)
        def _():
            g_copy(z, c, 1).start()

        for k in range(1, X):
            g_copy(z, c, k + 1).start()
        return carry

    lax.fori_loop(0, CHUNKS, update, 0)

    for s in range(1, Z):
        def relay(c, carry, s=s):
            @pl.when(z - s >= 0)
            def _():
                arrived(z - s, x, c)

                @pl.when(z < Z - 1)
                def _():
                    g_copy(z - s, c, 0).start()

                along_x(z - s, c, lambda copy: copy.start())

            @pl.when(z + s < Z)
            def _():
                arrived(z + s, x, c)

                @pl.when(z > 0)
                def _():
                    g_copy(z + s, c, 1).start()

                along_x(z + s, c, lambda copy: copy.start())

            return carry

        lax.fori_loop(0, CHUNKS, relay, 0)

        if s == 1:
            def across(c, carry):
                for k in range(1, X):
                    arrived(z, (x + k) % X, c)
                    h_copy(k, c).start()
                return carry

            lax.fori_loop(HALF, CHUNKS, across, 0)

    for s in range(Z):
        def collect(zz, s=s):
            def body(c, carry):
                for k in range(1, X):
                    arrived(zz, (x + k) % X, c)
                return carry

            lax.fori_loop(0, HALF if s == 0 else CHUNKS, body, 0)

        for_dest(s, collect)

    def drain(c, carry):
        for zz in range(Z):
            for k in range(1, X):
                x_copy(zz, k, c).wait_send()
            along_x(zz, c, lambda copy: copy.wait_send())

            @pl.when(zz > z)
            def _():
                z_copy(zz, c, True).wait_send()

            @pl.when(zz < z)
            def _():
                z_copy(zz, c, False).wait_send()

            @pl.when(jnp.logical_and(zz <= z, z < Z - 1))
            def _():
                g_copy(zz, c, 0).wait_send()

            @pl.when(jnp.logical_and(zz >= z, z > 0))
            def _():
                g_copy(zz, c, 1).wait_send()

        @pl.when(c >= HALF)
        def _():
            for k in range(1, X):
                h_copy(k, c).wait_send()

        return carry

    lax.fori_loop(0, CHUNKS, drain, 0)
    for k in range(1, n):
        n_copy(k).wait_send()
    for k in range(1, E):
        m_copy(k).wait_send()


def write_out(count, *refs):
    sources, targets, sem = refs[:count], refs[count : 2 * count], refs[2 * count]

    def copies(i):
        size = sources[i].shape[1] // PIECES
        for p in range(PIECES):
            where = pl.ds(p * size, size)
            yield pltpu.make_async_copy(sources[i].at[:, where], targets[i].at[:, where], sem.at[i, p])

    for i in range(count):
        for copy in copies(i):
            copy.start()
    for i in range(count):
        for copy in copies(i):
            copy.wait()


def split(count):
    rows = 1
    while rows * rows < count:
        rows *= 2
    return rows, count // rows


def shards(Z, X, E, local_grads, master_weights, first_moment, second_moment):
    layers, flat = local_grads.shape[2:]
    n = Z * X
    share = flat // n
    whole = pl.BlockSpec(memory_space=pltpu.HBM)
    piece = jax.ShapeDtypeStruct((layers, share), F32)
    dma = pltpu.SemaphoreType.DMA
    local = pl.BlockSpec(memory_space=pltpu.VMEM)
    shapes = (jax.ShapeDtypeStruct((layers, flat), jnp.bfloat16), piece, piece, piece)
    arrays = (local_grads[0, 0], master_weights[0], first_moment[0], second_moment[0])
    out_bytes = layers * (2 * flat + 3 * 4 * share)
    used_bytes = layers * Z * share * (2 * X + 3 * 4) + out_bytes
    results = pl.pallas_call(
        functools.partial(kernel, Z, X, E, share),
        out_shape=shapes,
        in_specs=[whole] * 4,
        out_specs=(local,) * 4,
        scratch_shapes=[
            pltpu.VMEM((Z, layers, share), jnp.bfloat16),
            pltpu.VMEM((Z, X - 1, layers, share), jnp.bfloat16),
            pltpu.VMEM((Z, layers, share), F32),
            pltpu.VMEM((Z, layers, share), F32),
            pltpu.VMEM((Z, layers, share), F32),
            pltpu.VMEM((n, 8, 128), F32),
            pltpu.VMEM((E, 8, 128), F32),
            dma((Z,)), dma((3,)),
            dma((Z, X - 1, CHUNKS)), dma((Z, X - 1, CHUNKS)),
            dma((Z, CHUNKS)), dma((Z, CHUNKS)), dma((Z, CHUNKS)),
            dma((n,)), dma((n,)), dma((E,)), dma((E,)),
            dma((X + 1, Z, CHUNKS)), dma((n, CHUNKS)), dma((X - 1, CHUNKS)),
        ],
        compiler_params=pltpu.CompilerParams(
            collective_id=0, has_side_effects=True, vmem_limit_bytes=used_bytes + SPARE_BYTES
        ),
    )(*(pltpu.with_memory_space_constraint(a, pltpu.HBM) for a in arrays))
    results = pl.pallas_call(
        functools.partial(write_out, len(shapes)),
        out_shape=shapes,
        in_specs=[local] * 4,
        out_specs=(whole,) * 4,
        scratch_shapes=[dma((len(shapes), PIECES))],
        compiler_params=pltpu.CompilerParams(vmem_limit_bytes=out_bytes + SPARE_BYTES),
    )(*results)
    return tuple(r[None] for r in results)


def solution(mesh):
    Z, X = split(mesh.shape["dp"])
    moments = P("expert", None, "dp")
    return jax.shard_map(
        functools.partial(shards, Z, X, mesh.shape["expert"]),
        mesh=mesh,
        in_specs=(P("dp", "expert", None, None), moments, moments, moments),
        out_specs=(P("expert", None, None), moments, moments, moments),
        check_vma=False,
    )
```
